32 devices in a mesh: owner: 16 (over z, y, core), rows: 2 (over x).
Axes of the slice: x: 2, y: 2, z: 4, core: 2. Of those that a mesh axis runs over, the one named last changes fastest.
Arguments:
- w_gate: float32 [64, 2048, 1024], P('owner', 'rows'), may hold values from -0.1875 to 0.1875
- avg_gate: float32 [64, 2048, 1024], P('owner', 'rows'), may hold values from -0.125 to 0.125
- w_up: float32 [64, 2048, 1024], P('owner', 'rows'), may hold values from -0.1875 to 0.1875
- avg_up: float32 [64, 2048, 1024], P('owner', 'rows'), may hold values from -0.125 to 0.125
- mix_share: float32 [64], P('owner'), may hold values from 0.2 to 0.8
- router_weight: float32 [2048, 64], P('rows', 'owner'), may hold values from -0.125 to 0.125
- router_gain: float32 [2048], P('rows'), may hold values from 0.25 to 1.75
Outputs:
- serve_gate: bfloat16 [64, 2048, 1024], P('owner')
- serve_up: bfloat16 [64, 2048, 1024], P('owner')
- scale_gate: float32 [64, 1024], P('owner')
- scale_up: float32 [64, 1024], P('owner')
- serve_router: bfloat16 [2048, 64], replicated
The draws below stay inside these ranges and needn't reach their ends.
All inputs are finite; a program needn't handle non-finite values.
Results may differ from the reference program's by a relative error of at most 0.0015.
Values may be sent and summed in bfloat16 or wider, within the bound.
A program may use at most 192 MiB of HBM per device.

```python
import jax
import jax.numpy as jnp
from jax import lax

EXPERTS = 64
D_MODEL = 2048
D_EXPERT = 1024


def raised(drawn, own_key, source, target, blocks, factor):
    def block_of(axis_at):
        return (jnp.arange(drawn.shape[axis_at]) // (drawn.shape[axis_at] // blocks)).reshape((-1,) + (1,) * (drawn.ndim - 1 - axis_at))

    near = jax.random.permutation(own_key, blocks)[block_of(target)]
    far = (block_of(target) + blocks // 2) % blocks
    return jnp.where((block_of(source) == near) | (block_of(source) == far), factor * drawn, drawn)


def level_of(key, shape, pieces, least, largest):
    factor_of = 1.0
    for position, blocks in pieces:
        heights = jax.random.uniform(jax.random.fold_in(jax.random.fold_in(key, 6), position), (blocks,), jnp.float32, least / len(pieces), largest / len(pieces))
        factor_of = factor_of * jnp.repeat(jnp.exp(heights), shape[position] // blocks).reshape((-1,) + (1,) * (len(shape) - 1 - position))
    return factor_of


def scatter_about(key, dims, width, most, cuts=(), held_as=jnp.bfloat16):
    drawn = jax.random.normal(key, dims, jnp.float32) * width
    if len(cuts) > 0:
        drawn = level_of(key, dims, cuts, -0.22, 0.18) * drawn
    return jnp.clip(drawn, min=-most, max=most).astype(held_as)


def heavy_noise(own_key, shape, spread, reach, split, heavy, kind=jnp.bfloat16):
    values = spread * jax.random.normal(own_key, shape, jnp.float32)
    if split:
        values = values * level_of(own_key, shape, split, -0.22, 0.18)
    return jnp.clip(raised(values, jax.random.fold_in(own_key, 3), *heavy), -reach, reach).astype(kind)


def setup_inputs(seed: int = 0) -> dict:
    key_of = jax.random.split(jax.random.key(seed), 8)
    w_gate = heavy_noise(key_of[0], (EXPERTS, D_MODEL, D_EXPERT), D_MODEL ** -0.5, 0.1875, ((0, 16), (1, 2)), (1, 2, 2, 2.0), jnp.float32)
    avg_gate = scatter_about(key_of[1], (EXPERTS, D_MODEL, D_EXPERT), D_MODEL ** -0.5, 0.125, ((0, 16), (1, 2)), jnp.float32)
    w_up = heavy_noise(key_of[2], (EXPERTS, D_MODEL, D_EXPERT), D_MODEL ** -0.5, 0.1875, ((0, 16), (1, 2)), (1, 2, 2, 2.0), jnp.float32)
    avg_up = scatter_about(key_of[3], (EXPERTS, D_MODEL, D_EXPERT), D_MODEL ** -0.5, 0.125, ((0, 16), (1, 2)), jnp.float32)
    mix_share = jnp.clip(0.2 + 0.6 * jax.random.uniform(key_of[4], (EXPERTS,), jnp.float32) ** level_of(key_of[4], (EXPERTS,), ((0, 16),), -0.2, 0.2), 0.2, 0.8)
    router_weight = scatter_about(key_of[5], (D_MODEL, EXPERTS), D_MODEL ** -0.5, 0.125, ((0, 2), (1, 16)), jnp.float32)
    router_gain = jnp.clip(1.0 + 0.15 * jax.random.normal(key_of[6], (D_MODEL,), jnp.float32), 0.25, 1.75)
    return {"w_gate": w_gate, "avg_gate": avg_gate, "w_up": w_up, "avg_up": avg_up, "mix_share": mix_share, "router_weight": router_weight, "router_gain": router_gain}


def reference(w_gate, avg_gate, w_up, avg_up, mix_share, router_weight, router_gain):
    fresh_gate = mix_share[:, None, None] * w_gate + (1.0 - mix_share[:, None, None]) * avg_gate
    fresh_up = mix_share[:, None, None] * w_up + (1.0 - mix_share[:, None, None]) * avg_up
    scale_gate = jnp.sqrt(lax.optimization_barrier(jnp.sum(fresh_gate * fresh_gate, axis=1)))
    serve_gate = (fresh_gate / jnp.expand_dims(scale_gate, 1)).astype(jnp.bfloat16)
    scale_up = jnp.sqrt(lax.optimization_barrier(jnp.sum(fresh_up * fresh_up, axis=1)))
    serve_up = (fresh_up / jnp.expand_dims(scale_up, 1)).astype(jnp.bfloat16)
    serve_router = (router_weight * router_gain[:, None]).astype(jnp.bfloat16)
    return (serve_gate, serve_up, scale_gate, scale_up, serve_router)
```

```python
import functools
import math

import jax
import jax.numpy as jnp
from jax import lax
from jax.experimental import pallas as pl
from jax.experimental.pallas import tpu as pltpu
from jax.sharding import PartitionSpec as P


ANY = pl.BlockSpec(memory_space=pl.ANY)
SMEM = pl.BlockSpec(memory_space=pltpu.SMEM)


def shift(x, n, k):
    return lax.ppermute(x, "rows", [((j + k) % n, j) for j in range(n)])


def halves_of(part, n):
    if n == 2:
        return part, shift(part, n, 1)
    if n == 1:
        return part, jnp.zeros_like(part)
    me = lax.axis_index("rows")
    stacked = jnp.stack([part] + [shift(part, n, k) for k in range(1, n)])
    total = jnp.zeros_like(part)
    for j in range(n):
        total = total + lax.dynamic_index_in_dim(stacked, lax.rem(j - me + n, n), 0, keepdims=False)
    return total, jnp.zeros_like(part)


def sum_kernel(first, share_ref, w_ref, avg_ref, dep_ref, out_ref):
    share = share_ref[pl.program_id(0) + first]
    fresh = share * w_ref[0] + (1.0 - share) * avg_ref[0]
    part = jnp.sum(fresh * fresh, axis=0, keepdims=True)[None]

    @pl.when(pl.program_id(1) == 0)
    def _():
        out_ref[...] = part

    @pl.when(pl.program_id(1) != 0)
    def _():
        out_ref[...] += part


def sums(share, w, avg, first, count, tile, dep):
    _, depth, width = w.shape
    spec = pl.BlockSpec((1, tile, width), lambda e, t: (e + first, t, 0))
    return pl.pallas_call(
        functools.partial(sum_kernel, first),
        grid=(count, depth // tile),
        in_specs=[SMEM, spec, spec, ANY],
        out_specs=pl.BlockSpec((1, 1, width), lambda e, t: (e, 0, 0)),
        out_shape=jax.ShapeDtypeStruct((count, 1, width), jnp.float32),
        cost_estimate=pl.CostEstimate(
            flops=5 * count * depth * width, bytes_accessed=8 * count * depth * width, transcendentals=0
        ),
    )(share, w, avg, dep)


def narrow_kernel(e, me_ref, share_ref, w_ref, avg_ref, a_ref, b_ref, *refs):
    send_ref, scale_ref, out_ref = refs[-3:]
    share = share_ref[e]
    fresh = share * w_ref[0] + (1.0 - share) * avg_ref[0]
    scale = jnp.sqrt(a_ref[0] + b_ref[0])
    served = (fresh / scale).astype(jnp.bfloat16)
    scale_ref[...] = scale
    send_ref[...] = served
    out_ref[0] = served


def narrow(me, share, w, avg, a, b, at, e, column, columns, n, tile, out, dep):
    experts, depth, width = w.shape
    tiles = depth // tile
    spec = pl.BlockSpec((1, tile, columns), lambda t, me: (e, t, column))
    sum_spec = pl.BlockSpec((1, 1, columns), lambda t, me: (at, 0, column))
    args = [share, w, avg, a, b, dep]
    in_specs = [SMEM, spec, spec, sum_spec, sum_spec, ANY]
    aliases = {}
    if out is not None:
        args.append(out)
        in_specs.append(ANY)
        aliases = {len(args): 2}
    return pl.pallas_call(
        functools.partial(narrow_kernel, e),
        grid_spec=pltpu.PrefetchScalarGridSpec(
            num_scalar_prefetch=1,
            grid=(tiles,),
            in_specs=in_specs,
            out_specs=[
                pl.BlockSpec((tile, columns), lambda t, me: (t, 0)),
                pl.BlockSpec((1, columns), lambda t, me: (0, 0)),
                pl.BlockSpec((1, tile, columns), lambda t, me: (e, me[0] * tiles + t, column)),
            ],
        ),
        out_shape=[
            jax.ShapeDtypeStruct((depth, columns), jnp.bfloat16),
            jax.ShapeDtypeStruct((1, columns), jnp.float32),
            jax.ShapeDtypeStruct((experts, n * depth, width), jnp.bfloat16),
        ],
        input_output_aliases=aliases,
        cost_estimate=pl.CostEstimate(
            flops=8 * depth * columns, bytes_accessed=12 * depth * columns, transcendentals=0
        ),
    )(me, *args)


def router_kernel(weight_ref, gain_ref, dep_ref, out_ref):
    out_ref[...] = (weight_ref[...] * gain_ref[...]).astype(jnp.bfloat16)


def router_part(weight, gain, dep):
    return pl.pallas_call(
        router_kernel,
        in_specs=[pl.BlockSpec(), pl.BlockSpec(), ANY],
        out_shape=jax.ShapeDtypeStruct(weight.shape, jnp.bfloat16),
        cost_estimate=pl.CostEstimate(flops=weight.size, bytes_accessed=8 * weight.size, transcendentals=0),
    )(weight, gain, dep)


def later_kernel(x_ref, dep_ref, out_ref):
    out_ref[...] = x_ref[...]


def later(x, dep):
    return pl.pallas_call(
        later_kernel,
        in_specs=[pl.BlockSpec(), ANY],
        out_shape=jax.ShapeDtypeStruct(x.shape, x.dtype),
        cost_estimate=pl.CostEstimate(flops=0, bytes_accessed=4 * x.size, transcendentals=0),
    )(x, dep)


def make_shards(n):
    def shards(w_gate, avg_gate, w_up, avg_up, mix_share, router_weight, router_gain):
        me = lax.axis_index("rows").astype(jnp.int32)
        at = me[None]
        experts, depth, width = w_gate.shape
        pairs = ((w_gate, avg_gate), (w_up, avg_up))
        tile = math.gcd(depth, 256)
        half = width // 2

        pieces = [(0, 0, 0, half), (0, 0, 1, half)]
        middle = [(which, e) for e in range(experts) for which in range(2)][1:]
        for which, e in middle[:-1]:
            pieces.append((which, e, 0, width))
        pieces += [(*middle[-1], 0, half), (*middle[-1], 1, half)]

        outs, scales, sends = [None, None], {}, []

        def send_piece(piece, halves, row, dep):
            which, e, column, columns = piece
            w, avg = pairs[which]
            send, scale, outs[which] = narrow(
                at, mix_share, w, avg, *halves, row, e, column, columns, n, tile, outs[which], dep
            )
            scales.setdefault((which, e), []).append(scale)
            sends.append((piece, [shift(send, n, k) for k in range(1, n)]))
            return send

        part = sums(mix_share, *pairs[0], 0, 1, tile, mix_share)
        router = router_part(router_weight.T, router_gain[None], part)
        halves = halves_of(part, n)
        sent = send_piece(pieces[0], halves, 0, part)

        held = {}
        last = sent
        if experts > 1:
            last = sums(mix_share, *pairs[0], 1, experts - 1, tile, last)
            held[0] = halves_of(last, n)
        last = sums(mix_share, *pairs[1], 0, experts, tile, last)
        held[1] = halves_of(last, n)

        last = send_piece(pieces[1], halves, 0, last)
        for piece in pieces[2:]:
            which, e = piece[:2]
            last = send_piece(piece, held[which], e if which else e - 1, last)

        moved = [shift(router, n, k) for k in range(1, n)]
        row_router = jnp.zeros((router.shape[0], n * depth), jnp.bfloat16)
        row_router = lax.dynamic_update_slice(row_router, router, (0, me * depth))
        for k in range(1, n):
            row_router = lax.dynamic_update_slice(
                row_router, moved[k - 1], (0, lax.rem(me + k, n) * depth)
            )
        serve_router = lax.all_gather(later(row_router, last), "owner", axis=0, tiled=True).T

        for (which, e, column, columns), got in sends:
            for k in range(1, n):
                outs[which] = lax.dynamic_update_slice(
                    outs[which], got[k - 1][None], (e, lax.rem(me + k, n) * depth, column * columns)
                )

        scale_gate, scale_up = (
            jnp.concatenate([jnp.concatenate(scales[which, e], axis=1) for e in range(experts)], axis=0)
            for which in range(2)
        )
        return (outs[0], outs[1], scale_gate, scale_up, serve_router)

    return shards


def solution(mesh):
    placed = (
        P("owner", "rows", None),
        P("owner", "rows", None),
        P("owner", "rows", None),
        P("owner", "rows", None),
        P("owner"),
        P("rows", "owner"),
        P("rows"),
    )
    return jax.shard_map(
        make_shards(mesh.shape["rows"]),
        mesh=mesh,
        in_specs=placed,
        out_specs=(
            P("owner", None, None),
            P("owner", None, None),
            P("owner", None),
            P("owner", None),
            P(),
        ),
        check_vma=False,
    )
```

```python
import functools
import math

import jax
import jax.numpy as jnp
from jax import lax
from jax.experimental import pallas as pl
from jax.experimental.pallas import tpu as pltpu
from jax.sharding import PartitionSpec as P


ANY = pl.BlockSpec(memory_space=pl.ANY)
SMEM = pl.BlockSpec(memory_space=pltpu.SMEM)


def shift(x, n, k):
    return lax.ppermute(x, "rows", [((j + k) % n, j) for j in range(n)])


def halves_of(part, n):
    if n == 2:
        return part, shift(part, n, 1)
    if n == 1:
        return part, jnp.zeros_like(part)
    me = lax.axis_index("rows")
    stacked = jnp.stack([part] + [shift(part, n, k) for k in range(1, n)])
    total = jnp.zeros_like(part)
    for j in range(n):
        total = total + lax.dynamic_index_in_dim(stacked, lax.rem(j - me + n, n), 0, keepdims=False)
    return total, jnp.zeros_like(part)


def sum_kernel(first, share_ref, w_ref, avg_ref, dep_ref, out_ref):
    share = share_ref[pl.program_id(0) + first]
    fresh = share * w_ref[0] + (1.0 - share) * avg_ref[0]
    part = jnp.sum(fresh * fresh, axis=0, keepdims=True)[None]

    @pl.when(pl.program_id(1) == 0)
    def _():
        out_ref[...] = part

    @pl.when(pl.program_id(1) != 0)
    def _():
        out_ref[...] += part


def sums(share, w, avg, first, count, tile, dep):
    _, depth, width = w.shape
    spec = pl.BlockSpec((1, tile, width), lambda e, t: (e + first, t, 0))
    return pl.pallas_call(
        functools.partial(sum_kernel, first),
        grid=(count, depth // tile),
        in_specs=[SMEM, spec, spec, ANY],
        out_specs=pl.BlockSpec((1, 1, width), lambda e, t: (e, 0, 0)),
        out_shape=jax.ShapeDtypeStruct((count, 1, width), jnp.float32),
        cost_estimate=pl.CostEstimate(
            flops=5 * count * depth * width, bytes_accessed=8 * count * depth * width, transcendentals=0
        ),
    )(share, w, avg, dep)


def narrow_kernel(e, me_ref, share_ref, w_ref, avg_ref, a_ref, b_ref, *refs):
    send_ref, scale_ref, out_ref = refs[-3:]
    share = share_ref[e]
    fresh = share * w_ref[0] + (1.0 - share) * avg_ref[0]
    scale = jnp.sqrt(a_ref[0] + b_ref[0])
    served = (fresh / scale).astype(jnp.bfloat16)
    scale_ref[...] = scale
    send_ref[...] = served
    out_ref[0] = served


def narrow(me, share, w, avg, a, b, at, e, column, columns, n, tile, out, dep):
    experts, depth, width = w.shape
    tiles = depth // tile
    spec = pl.BlockSpec((1, tile, columns), lambda t, me: (e, t, column))
    sum_spec = pl.BlockSpec((1, 1, columns), lambda t, me: (at, 0, column))
    args = [share, w, avg, a, b, dep]
    in_specs = [SMEM, spec, spec, sum_spec, sum_spec, ANY]
    aliases = {}
    if out is not None:
        args.append(out)
        in_specs.append(ANY)
        aliases = {len(args): 2}
    return pl.pallas_call(
        functools.partial(narrow_kernel, e),
        grid_spec=pltpu.PrefetchScalarGridSpec(
            num_scalar_prefetch=1,
            grid=(tiles,),
            in_specs=in_specs,
            out_specs=[
                pl.BlockSpec((tile, columns), lambda t, me: (t, 0)),
                pl.BlockSpec((1, columns), lambda t, me: (0, 0)),
                pl.BlockSpec((1, tile, columns), lambda t, me: (e, me[0] * tiles + t, column)),
            ],
        ),
        out_shape=[
            jax.ShapeDtypeStruct((depth, columns), jnp.bfloat16),
            jax.ShapeDtypeStruct((1, columns), jnp.float32),
            jax.ShapeDtypeStruct((experts, n * depth, width), jnp.bfloat16),
        ],
        input_output_aliases=aliases,
        cost_estimate=pl.CostEstimate(
            flops=8 * depth * columns, bytes_accessed=12 * depth * columns, transcendentals=0
        ),
    )(me, *args)


def router_kernel(weight_ref, gain_ref, dep_ref, out_ref):
    out_ref[...] = (weight_ref[...] * gain_ref[...]).astype(jnp.bfloat16)


def router_part(weight, gain, dep):
    return pl.pallas_call(
        router_kernel,
        in_specs=[pl.BlockSpec(), pl.BlockSpec(), ANY],
        out_shape=jax.ShapeDtypeStruct(weight.shape, jnp.bfloat16),
        cost_estimate=pl.CostEstimate(flops=weight.size, bytes_accessed=8 * weight.size, transcendentals=0),
    )(weight, gain, dep)


def later_kernel(x_ref, dep_ref, out_ref):
    out_ref[...] = x_ref[...]


def later(x, dep):
    return pl.pallas_call(
        later_kernel,
        in_specs=[pl.BlockSpec(), ANY],
        out_shape=jax.ShapeDtypeStruct(x.shape, x.dtype),
        cost_estimate=pl.CostEstimate(flops=0, bytes_accessed=4 * x.size, transcendentals=0),
    )(x, dep)


def make_shards(n):
    def shards(w_gate, avg_gate, w_up, avg_up, mix_share, router_weight, router_gain):
        me = lax.axis_index("rows").astype(jnp.int32)
        at = me[None]
        experts, depth, width = w_gate.shape
        pairs = ((w_gate, avg_gate), (w_up, avg_up))
        tile, tall = math.gcd(depth, 256), math.gcd(depth, 512)
        half = width // 2

        pieces = [(0, 0, 0, half), (0, 0, 1, half)]
        middle = [(which, e) for e in range(experts) for which in range(2)][1:]
        for which, e in middle[:-1]:
            pieces.append((which, e, 0, width))
        pieces += [(*middle[-1], 0, half), (*middle[-1], 1, half)]

        outs, scales, sends = [None, None], {}, []

        def send_piece(piece, halves, row, dep):
            which, e, column, columns = piece
            w, avg = pairs[which]
            send, scale, outs[which] = narrow(
                at, mix_share, w, avg, *halves, row, e, column, columns, n, tile, outs[which], dep
            )
            scales.setdefault((which, e), []).append(scale)
            sends.append((piece, [shift(send, n, k) for k in range(1, n)]))
            return send

        part = sums(mix_share, *pairs[0], 0, 1, tile, mix_share)
        router = router_part(router_weight.T, router_gain[None], part)
        halves = halves_of(part, n)
        sent = send_piece(pieces[0], halves, 0, part)

        held = {}

        def sum_rest(which, first, count, dep):
            part = sums(mix_share, *pairs[which], first, count, tall, dep)
            got = halves_of(part, n)
            for i in range(count):
                held[which, first + i] = (got, i)
            return part

        last = sum_rest(1, 0, 1, sent)
        last = send_piece(pieces[1], halves, 0, last)
        if experts > 1:
            last = sum_rest(0, 1, experts - 1, last)
        for i, piece in enumerate(pieces[2:]):
            last = send_piece(piece, *held[piece[:2]], last)
            if i == 0 and experts > 1:
                last = sum_rest(1, 1, experts - 1, last)

        moved = [shift(router, n, k) for k in range(1, n)]
        row_router = jnp.zeros((router.shape[0], n * depth), jnp.bfloat16)
        row_router = lax.dynamic_update_slice(row_router, router, (0, me * depth))
        for k in range(1, n):
            row_router = lax.dynamic_update_slice(
                row_router, moved[k - 1], (0, lax.rem(me + k, n) * depth)
            )
        serve_router = lax.all_gather(later(row_router, last), "owner", axis=0, tiled=True).T

        for (which, e, column, columns), got in sends:
            for k in range(1, n):
                outs[which] = lax.dynamic_update_slice(
                    outs[which], got[k - 1][None], (e, lax.rem(me + k, n) * depth, column * columns)
                )

        scale_gate, scale_up = (
            jnp.concatenate([jnp.concatenate(scales[which, e], axis=1) for e in range(experts)], axis=0)
            for which in range(2)
        )
        return (outs[0], outs[1], scale_gate, scale_up, serve_router)

    return shards


def solution(mesh):
    placed = (
        P("owner", "rows", None),
        P("owner", "rows", None),
        P("owner", "rows", None),
        P("owner", "rows", None),
        P("owner"),
        P("rows", "owner"),
        P("rows"),
    )
    return jax.shard_map(
        make_shards(mesh.shape["rows"]),
        mesh=mesh,
        in_specs=placed,
        out_specs=(
            P("owner", None, None),
            P("owner", None, None),
            P("owner", None),
            P("owner", None),
            P(),
        ),
        check_vma=False,
    )
```
